256 devices in a mesh: col: 32 (over z, y), row: 8 (over x, core).
Axes of the slice: x: 4, y: 4, z: 8, core: 2. Of those that a mesh axis runs over, the one named last changes fastest.
Arguments:
- f_rhs: float32 [256, 1024, 96], P('row', 'col')
- u_init: float32 [256, 1024, 96], P('row', 'col')
- kappa_cell: float32 [256, 1024], P('row', 'col')
- solve_mats: bfloat16 [8, 32, 1024, 2304], P('row', 'col')
- omega_relax: float32 [], replicated
Outputs:
- output: float32 [256, 1024, 96], P('row', 'col')
All inputs are finite; a program needn't handle non-finite values.
Results may differ from the reference program's by a relative error of at most 0.00191557.
Values are sent between devices in bfloat16 or wider.
A program may use at most 768 MiB of HBM per device.

```python
import jax
import jax.numpy as jnp
from jax import lax

SUB_SIZE = 32
MARGIN = 8
RHS_COUNT = 96
ROW_BLOCKS = 8
COL_BLOCKS = 32
SWEEPS = 6

EXT_SIZE = SUB_SIZE + 2 * MARGIN
GRID_ROWS = SUB_SIZE * ROW_BLOCKS
GRID_COLS = SUB_SIZE * COL_BLOCKS


def face_coeffs(kappa_cell):
    inner_v = 0.5 * (kappa_cell[1:, :] + kappa_cell[:-1, :])
    inner_h = 0.5 * (kappa_cell[:, 1:] + kappa_cell[:, :-1])
    face_n = jnp.concatenate([kappa_cell[:1, :], inner_v], axis=0)
    face_s = jnp.concatenate([inner_v, kappa_cell[-1:, :]], axis=0)
    face_w = jnp.concatenate([kappa_cell[:, :1], inner_h], axis=1)
    face_e = jnp.concatenate([inner_h, kappa_cell[:, -1:]], axis=1)
    return face_n, face_s, face_w, face_e


def apply_operator(values, face_set):
    face_n, face_s, face_w, face_e = face_set
    padded = jnp.pad(values, ((1, 1), (1, 1), (0, 0)))
    diag_sum = (face_n + face_s + face_w + face_e)[:, :, None]
    return (diag_sum * values
            - face_n[:, :, None] * padded[:-2, 1:-1]
            - face_s[:, :, None] * padded[2:, 1:-1]
            - face_w[:, :, None] * padded[1:-1, :-2]
            - face_e[:, :, None] * padded[1:-1, 2:])


def build_solve_mats(kappa_cell):
    face_n, face_s, face_w, face_e = face_coeffs(kappa_cell)
    diag_sum = face_n + face_s + face_w + face_e
    link_s = jnp.concatenate([face_s[:-1, :], jnp.zeros((1, GRID_COLS), jnp.float32)], axis=0)
    link_e = jnp.concatenate([face_e[:, :-1], jnp.zeros((GRID_ROWS, 1), jnp.float32)], axis=1)
    pad_cfg = ((MARGIN, MARGIN), (MARGIN, MARGIN))
    diag_pad = jnp.pad(diag_sum, pad_cfg, constant_values=1.0)
    south_pad = jnp.pad(link_s, pad_cfg)
    east_pad = jnp.pad(link_e, pad_cfg)
    ext_cells = EXT_SIZE * EXT_SIZE
    col_mask = (jnp.arange(EXT_SIZE) < EXT_SIZE - 1).astype(jnp.float32)

    def one_block(block_idx):
        corner_at = (block_idx // COL_BLOCKS * SUB_SIZE, block_idx % COL_BLOCKS * SUB_SIZE)
        diag_w = lax.dynamic_slice(diag_pad, corner_at, (EXT_SIZE, EXT_SIZE)).reshape(ext_cells)
        south_w = lax.dynamic_slice(south_pad, corner_at, (EXT_SIZE, EXT_SIZE)).reshape(ext_cells)
        east_w = (lax.dynamic_slice(east_pad, corner_at, (EXT_SIZE, EXT_SIZE)) * col_mask[None, :]).reshape(ext_cells)
        local_op = (jnp.diag(diag_w)
                    - jnp.diag(east_w[:-1], 1) - jnp.diag(east_w[:-1], -1)
                    - jnp.diag(south_w[:-EXT_SIZE], EXT_SIZE) - jnp.diag(south_w[:-EXT_SIZE], -EXT_SIZE))
        inverse = jnp.linalg.inv(local_op).reshape(EXT_SIZE, EXT_SIZE, ext_cells)
        rows_kept = inverse[MARGIN:MARGIN + SUB_SIZE, MARGIN:MARGIN + SUB_SIZE]
        return rows_kept.reshape(SUB_SIZE * SUB_SIZE, ext_cells)

    all_mats = lax.map(one_block, jnp.arange(ROW_BLOCKS * COL_BLOCKS))
    return all_mats.reshape(ROW_BLOCKS, COL_BLOCKS, SUB_SIZE * SUB_SIZE, ext_cells).astype(jnp.bfloat16)


def setup_inputs(seed: int = 0) -> dict:
    root_key = jax.random.key(seed)
    key_rhs, key_init, key_coef, key_omega = jax.random.split(root_key, 4)
    rhs_scale = 16.0 / (EXT_SIZE * EXT_SIZE)
    grid_shape = (GRID_ROWS, GRID_COLS, RHS_COUNT)
    f_rhs = rhs_scale * (1.0 + jax.random.normal(key_rhs, grid_shape, jnp.float32))
    u_init = jax.random.normal(key_init, grid_shape, jnp.float32)
    kappa_cell = jnp.exp(jax.random.uniform(key_coef, (GRID_ROWS, GRID_COLS), jnp.float32, -0.8, 0.8))
    omega_relax = jax.random.uniform(key_omega, (), jnp.float32, 0.7, 1.0)
    return dict(f_rhs=f_rhs, u_init=u_init, kappa_cell=kappa_cell,
                solve_mats=build_solve_mats(kappa_cell), omega_relax=omega_relax)


def local_solves(residual, solve_mats):
    padded = jnp.pad(residual.astype(jnp.bfloat16), ((MARGIN, MARGIN), (MARGIN, MARGIN), (0, 0)))

    def one_block(block_idx):
        blk_row = block_idx // COL_BLOCKS
        blk_col = block_idx % COL_BLOCKS
        window = lax.dynamic_slice(padded, (blk_row * SUB_SIZE, blk_col * SUB_SIZE, 0),
                                   (EXT_SIZE, EXT_SIZE, RHS_COUNT))
        product = jnp.dot(solve_mats[blk_row, blk_col], window.reshape(EXT_SIZE * EXT_SIZE, RHS_COUNT),
                          preferred_element_type=jnp.float32)
        return product.astype(jnp.bfloat16)

    blocks = lax.map(one_block, jnp.arange(ROW_BLOCKS * COL_BLOCKS))
    blocks = blocks.reshape(ROW_BLOCKS, COL_BLOCKS, SUB_SIZE, SUB_SIZE, RHS_COUNT)
    return blocks.transpose(0, 2, 1, 3, 4).reshape(GRID_ROWS, GRID_COLS, RHS_COUNT)


def reference(f_rhs, u_init, kappa_cell, solve_mats, omega_relax):
    face_set = face_coeffs(kappa_cell)
    residual = f_rhs - apply_operator(u_init, face_set)

    def one_sweep(state_pair, unused):
        u_cur, res_cur = state_pair
        correction = local_solves(res_cur, solve_mats).astype(jnp.float32)
        u_next = u_cur + omega_relax * correction
        res_next = res_cur - omega_relax * apply_operator(correction, face_set)
        return (u_next, res_next), None

    final_pair, unused_out = lax.scan(one_sweep, (u_init, residual), None, length=SWEEPS)
    return final_pair[0]
```

```python
import functools
import math
import jax
import jax.numpy as jnp
from jax import lax
from jax.experimental import pallas as pl
from jax.experimental.pallas import tpu as pltpu
from jax.sharding import PartitionSpec as P

SWEEPS = 6
MESH = pl.DeviceIdType.MESH
DIRS = ((-1, 0), (1, 0), (0, -1), (0, 1), (-1, -1), (-1, 1), (1, -1), (1, 1))
BACK = (1, 0, 3, 2, 7, 6, 5, 4)
N, S, W, E, NW, NE, SW, SE = range(8)
F32, BF16 = jnp.float32, jnp.bfloat16


def kernel(geo, omega_ref, f_hbm, u_hbm, k_hbm, a_hbm, out_hbm,
           mat, u, r, ext, zf, cs, cw, ce, kp, kraw, knb,
           ucol, urow_in, ucol_in,
           zo, st_e, st_w, st_c, h_n, h_s, h_w, h_e, h_c,
           load_sem, u_send, u_recv, k_send, k_recv, r_send, r_recv, z_send, z_recv):
    row_count, col_count, sub, halo, rhs = geo
    big = sub + 2 * halo
    tiles = sub // 8
    row, col = lax.axis_index('row'), lax.axis_index('col')
    omega = omega_ref[0, 0]

    def exists(d):
        dr, dc = DIRS[d]
        conds = []
        if dr == -1:
            conds.append(row > 0)
        if dr == 1:
            conds.append(row < row_count - 1)
        if dc == -1:
            conds.append(col > 0)
        if dc == 1:
            conds.append(col < col_count - 1)
        return functools.reduce(jnp.logical_and, conds)

    def device(d):
        dr, dc = DIRS[d]
        return {'row': row + dr, 'col': col + dc}

    def each(fn, dirs=range(8)):
        for d in dirs:
            pl.when(exists(d))(functools.partial(fn, d))

    loads = [pltpu.make_async_copy(k_hbm, kraw, load_sem.at[0]),
             pltpu.make_async_copy(u_hbm, u, load_sem.at[1]),
             pltpu.make_async_copy(f_hbm, r.at[pl.ds(halo, sub), pl.ds(halo, sub)], load_sem.at[2]),
             pltpu.make_async_copy(a_hbm, mat, load_sem.at[3])]
    for copy in loads:
        copy.start()

    for start in (0, halo + sub):
        r[pl.ds(start, halo)] = jnp.zeros((halo, big, rhs), F32)
        r[pl.ds(halo, sub), pl.ds(start, halo)] = jnp.zeros((sub, halo, rhs), F32)
    knb[...] = jnp.zeros_like(knb)

    barrier = pltpu.get_barrier_semaphore()

    def greet(d):
        pl.semaphore_signal(barrier, inc=1, device_id=device(d), device_id_type=MESH)

    each(greet)

    def zero_row(i, carry):
        zf[i] = jnp.zeros((big + 16, rhs), F32)
        return carry

    lax.fori_loop(0, big + 2, zero_row, 0)
    kp[...] = jnp.zeros_like(kp)
    loads[0].wait()
    kp[:, 0:sub] = kraw[...]
    loads[1].wait()

    def u_to_zf(i, carry):
        zf[halo + 1 + i, pl.ds(halo + 8, sub)] = u[pl.ds(pl.multiple_of(i * sub, sub), sub)]
        return carry

    lax.fori_loop(0, sub, u_to_zf, 0)
    ucol[0] = zf[pl.ds(halo + 1, sub), halo + 8, :]
    ucol[1] = zf[pl.ds(halo + 1, sub), halo + 8 + sub - 1, :]

    def band(at, count):
        return 3 - (at == 0).astype(jnp.int32) - (at == count - 1).astype(jnp.int32)

    pl.semaphore_wait(barrier, band(row, row_count) * band(col, col_count) - 1)

    def u_copy(d):
        src = {N: u.at[pl.ds(0, sub)], S: u.at[pl.ds((sub - 1) * sub, sub)],
               W: ucol.at[0], E: ucol.at[1]}[d]
        dst = {N: urow_in.at[1], S: urow_in.at[0], W: ucol_in.at[1], E: ucol_in.at[0]}[d]
        return pltpu.make_async_remote_copy(src, dst, u_send.at[d], u_recv.at[BACK[d]],
                                            device_id=device(d), device_id_type=MESH)

    def u_arrival(d):
        dst = {N: urow_in.at[0], S: urow_in.at[1], W: ucol_in.at[0], E: ucol_in.at[1]}[d]
        return pltpu.make_async_remote_copy(dst, dst, u_send.at[d], u_recv.at[d],
                                            device_id=device(d), device_id_type=MESH)

    def k_copy(d):
        return pltpu.make_async_remote_copy(kp, knb.at[BACK[d]], k_send.at[d], k_recv.at[BACK[d]],
                                            device_id=device(d), device_id_type=MESH)

    def k_arrival(d):
        return pltpu.make_async_remote_copy(knb.at[d], knb.at[d], k_send.at[d], k_recv.at[d],
                                            device_id=device(d), device_id_type=MESH)

    each(lambda d: u_copy(d).start(), (E, W, S, N))
    each(lambda d: k_copy(d).start(), (E, W, S, N, NE, NW, SE, SW))
    each(lambda d: k_arrival(d).wait_recv())

    def block_row(left, mid, right):
        return left + pltpu.roll(mid, sub, 1) + pltpu.roll(right, 2 * sub, 1)

    kk = jnp.concatenate([block_row(knb[NW], knb[N], knb[NE]),
                          block_row(knb[W], kp[...], knb[E]),
                          block_row(knb[SW], knb[S], knb[SE]),
                          jnp.zeros((128 - 3 * sub, 128), F32)], axis=0)
    kt = jnp.transpose(kk)
    g_row = row * sub - sub + lax.broadcasted_iota(jnp.int32, (128, 128), 1)
    g_col = col * sub - sub + lax.broadcasted_iota(jnp.int32, (128, 128), 0)
    row_in = jnp.logical_and(g_row >= 0, g_row < row_count * sub)
    col_in = jnp.logical_and(g_col >= 0, g_col < col_count * sub)
    row_next = jnp.logical_and(g_row >= -1, g_row < row_count * sub - 1)
    col_next = jnp.logical_and(g_col >= -1, g_col < col_count * sub - 1)
    here = jnp.logical_and(row_in, col_in)
    kt = jnp.where(here, kt, 0.0)
    k_down = pltpu.roll(kt, 127, 1)
    k_right = pltpu.roll(kt, 127, 0)
    face_s = jnp.where(jnp.logical_and(here, jnp.logical_and(row_next, col_in)), 0.5, 1.0) * (kt + k_down)
    face_e = jnp.where(jnp.logical_and(here, jnp.logical_and(row_in, col_next)), 0.5, 1.0) * (kt + k_right)
    face_w = pltpu.roll(face_e, 1, 0)
    j0 = sub - halo
    for i in range(-1, big):
        lane = i + sub - halo
        cs[i + 1] = jnp.broadcast_to(face_s[j0:j0 + big, lane:lane + 1], (big, rhs))
        if i >= 0:
            cw[i] = jnp.broadcast_to(face_w[j0:j0 + big, lane:lane + 1], (big, rhs))
            ce[i] = jnp.broadcast_to(face_e[j0:j0 + big, lane:lane + 1], (big, rhs))

    def operator(i, j, width):
        c = zf[i + 1, pl.ds(8 + j, width)]
        span = pl.ds(j, width)
        return (cs[i, span] * (c - zf[i, pl.ds(8 + j, width)])
                + cs[i + 1, span] * (c - zf[i + 2, pl.ds(8 + j, width)])
                + cw[i, span] * (c - zf[i + 1, pl.ds(7 + j, width)])
                + ce[i, span] * (c - zf[i + 1, pl.ds(9 + j, width)]))

    def put_u(d):
        u_arrival(d).wait_recv()
        if d == N:
            zf[halo, pl.ds(halo + 8, sub)] = urow_in[0]
        if d == S:
            zf[halo + sub + 1, pl.ds(halo + 8, sub)] = urow_in[1]
        if d == W:
            zf[pl.ds(halo + 1, sub), halo + 7, :] = ucol_in[0]
        if d == E:
            zf[pl.ds(halo + 1, sub), halo + 8 + sub, :] = ucol_in[1]

    each(put_u, (N, S, W, E))
    loads[2].wait()

    def first_residual(i, carry):
        r[i, pl.ds(halo, sub)] = r[i, pl.ds(halo, sub)] - operator(i, halo, sub)
        return carry

    lax.fori_loop(halo, halo + sub, first_residual, 0)

    def span_of(delta, outer):
        if delta == 0:
            return pl.ds(halo, sub)
        if outer:
            return pl.ds(0, halo) if delta < 0 else pl.ds(halo + sub, halo)
        return pl.ds(halo, halo) if delta < 0 else pl.ds(sub, halo)

    def r_copy(d):
        dr, dc = DIRS[d]
        return pltpu.make_async_remote_copy(
            r.at[span_of(dr, False), span_of(dc, False)], r.at[span_of(-dr, True), span_of(-dc, True)],
            r_send.at[d], r_recv.at[BACK[d]], device_id=device(d), device_id_type=MESH)

    def r_arrival(d):
        dr, dc = DIRS[d]
        dst = r.at[span_of(dr, True), span_of(dc, True)]
        return pltpu.make_async_remote_copy(dst, dst, r_send.at[d], r_recv.at[d],
                                            device_id=device(d), device_id_type=MESH)

    each(lambda d: r_copy(d).start(), (E, W, NE, NW, SE, SW, S, N))
    each(lambda d: u_copy(d).wait_send(), (N, S, W, E))
    each(lambda d: k_copy(d).wait_send())
    loads[3].wait()
    each(lambda d: r_copy(d).wait_send())
    each(lambda d: r_arrival(d).wait_recv())

    def round_row(i, carry):
        ext[i] = r[i].astype(BF16)
        return carry

    lax.fori_loop(0, big, round_row, 0)

    def solve(chunk, e):
        z = jnp.dot(mat[pl.ds(chunk * 8 * sub, 8 * sub), :], e, preferred_element_type=F32)
        return z.astype(BF16).astype(F32)

    def z_source(d, slot):
        return {N: zo.at[slot, pl.ds(0, halo + 1)], S: zo.at[slot, pl.ds(sub - halo - 1, halo + 1)],
                W: st_w.at[slot], E: st_e.at[slot]}.get(d, st_c.at[slot, d - 4] if d >= 4 else None)

    def z_place(d, slot):
        return {N: h_n.at[slot], S: h_s.at[slot], W: h_w.at[slot], E: h_e.at[slot]}.get(
            d, h_c.at[slot, d - 4] if d >= 4 else None)

    def z_copy(d, slot):
        return pltpu.make_async_remote_copy(
            z_source(d, slot), z_place(BACK[d], slot), z_send.at[slot, d], z_recv.at[slot, BACK[d]],
            device_id=device(d), device_id_type=MESH)

    def z_arrival(d, slot):
        return pltpu.make_async_remote_copy(
            z_place(d, slot), z_place(d, slot), z_send.at[slot, d], z_recv.at[slot, d],
            device_id=device(d), device_id_type=MESH)

    left_col, right_col = halo, sub - halo - 1
    low, high = pl.ds(0, halo + 1), pl.ds(sub - halo - 1, halo + 1)

    def sweep(t, carry):
        slot = lax.rem(t, 2)
        e = ext[...].reshape(big * big, rhs)
        for chunk in range(sub // 8):
            z = solve(chunk, e)
            rows = pl.ds(8 * chunk, 8)
            zf[pl.ds(halo + 1 + 8 * chunk, 8), pl.ds(halo + 8, sub)] = z.reshape(8, sub, rhs)
            zb = z.reshape(8, tiles, 8, rhs).astype(BF16)
            zo[slot, rows] = zb
            st_w[slot, rows] = zb[:, 0]
            st_e[slot, rows] = zb[:, tiles - 1]
            st_w[slot, sub + chunk] = zf[pl.ds(halo + 1 + 8 * chunk, 8), halo + 8 + left_col, :].astype(BF16)
            st_e[slot, sub + chunk] = zf[pl.ds(halo + 1 + 8 * chunk, 8), halo + 8 + right_col, :].astype(BF16)
        for d, strip, rows, extra in ((NW, st_w, low, 0), (NE, st_e, low, 0),
                                      (SW, st_w, high, tiles - 1), (SE, st_e, high, tiles - 1)):
            st_c[slot, d - 4, pl.ds(0, halo + 1)] = strip[slot, rows]
            st_c[slot, d - 4, halo + 1] = strip[slot, sub + extra]
        each(lambda d: z_copy(d, slot).start(), (E, W, NE, NW, SE, SW, S, N))

        def add_u(i, c):
            cells = pl.ds(pl.multiple_of(i * sub, sub), sub)
            u[cells] = u[cells] + omega * zf[halo + 1 + i, pl.ds(halo + 8, sub)]
            return c

        lax.fori_loop(0, sub, add_u, 0)
        right, below = halo + sub + 8, halo + sub + 1

        def put_z(d):
            z_arrival(d, slot).wait_recv()
            if d in (N, S):
                buf, at = (h_n, 0) if d == N else (h_s, below)
                zf[pl.ds(at, halo + 1), pl.ds(halo + 8, sub)] = buf[slot].astype(F32).reshape(halo + 1, sub, rhs)
            elif d in (W, E):
                buf, at, edge = (h_w, 8, 7) if d == W else (h_e, right, right + 8)
                zf[pl.ds(halo + 1, sub), pl.ds(at, 8)] = buf[slot, pl.ds(0, sub)].astype(F32)
                for k in range(tiles):
                    zf[pl.ds(halo + 1 + 8 * k, 8), edge, :] = buf[slot, sub + k].astype(F32)
            else:
                dr, dc = DIRS[d]
                at, edge = (8, 7) if dc < 0 else (right, right + 8)
                start, edge_start = (0, 1) if dr < 0 else (below, below)
                zf[pl.ds(start, halo + 1), pl.ds(at, 8)] = h_c[slot, d - 4, pl.ds(0, halo + 1)].astype(F32)
                zf[pl.ds(edge_start, 8), edge, :] = h_c[slot, d - 4, halo + 1].astype(F32)

        each(put_z)

        def update(i, c):
            new = r[i] - omega * operator(i, 0, big)
            r[i] = new
            ext[i] = new.astype(BF16)
            return c

        lax.fori_loop(0, big, update, 0)
        each(lambda d: z_copy(d, slot).wait_send())
        return carry

    lax.fori_loop(0, SWEEPS - 1, sweep, 0)
    e = ext[...].reshape(big * big, rhs)
    for chunk in range(sub // 8):
        cells = pl.ds(chunk * 8 * sub, 8 * sub)
        u[cells] = u[cells] + omega * solve(chunk, e)
    done = pltpu.make_async_copy(u, out_hbm, load_sem.at[0])
    done.start()
    done.wait()


def solution(mesh):
    row_count = mesh.shape['row']
    col_count = mesh.shape['col']
    grid_spec = P('row', 'col', None)

    def device_fn(f_blk, u_blk, kappa_blk, mat_blk, omega_relax):
        sub, _, rhs = u_blk.shape
        rows, cols = mat_blk.shape[2:]
        big = math.isqrt(cols)
        halo = (big - sub) // 2
        tiles = sub // 8
        dma, vmem = pltpu.SemaphoreType.DMA, pltpu.VMEM
        out = pl.pallas_call(
            functools.partial(kernel, (row_count, col_count, sub, halo, rhs)),
            out_shape=jax.ShapeDtypeStruct((sub * sub, rhs), F32),
            in_specs=[pl.BlockSpec(memory_space=pltpu.SMEM)] + [pl.BlockSpec(memory_space=pl.ANY)] * 4,
            out_specs=pl.BlockSpec(memory_space=pl.ANY),
            scratch_shapes=[
                vmem((rows, cols), BF16), vmem((sub * sub, rhs), F32), vmem((big, big, rhs), F32),
                vmem((big, big, rhs), BF16), vmem((big + 2, big + 16, rhs), F32),
                vmem((big + 1, big, rhs), F32), vmem((big, big, rhs), F32), vmem((big, big, rhs), F32),
                vmem((sub, 128), F32), vmem((sub, sub), F32), vmem((8, sub, 128), F32),
                vmem((2, sub, rhs), F32), vmem((2, sub, rhs), F32), vmem((2, sub, rhs), F32),
                vmem((2, sub, tiles, 8, rhs), BF16),
                vmem((2, sub + tiles, 8, rhs), BF16), vmem((2, sub + tiles, 8, rhs), BF16),
                vmem((2, 4, halo + 2, 8, rhs), BF16),
                vmem((2, halo + 1, tiles, 8, rhs), BF16), vmem((2, halo + 1, tiles, 8, rhs), BF16),
                vmem((2, sub + tiles, 8, rhs), BF16), vmem((2, sub + tiles, 8, rhs), BF16),
                vmem((2, 4, halo + 2, 8, rhs), BF16),
                dma((4,)), dma((4,)), dma((4,)), dma((8,)), dma((8,)), dma((8,)), dma((8,)),
                dma((2, 8)), dma((2, 8)),
            ],
            compiler_params=pltpu.CompilerParams(collective_id=0, has_side_effects=True),
        )(omega_relax.reshape(1, 1), f_blk, u_blk.reshape(sub * sub, rhs), kappa_blk, mat_blk.reshape(rows, cols))
        return out.reshape(sub, sub, rhs)

    return jax.shard_map(device_fn, mesh=mesh,
                         in_specs=(grid_spec, grid_spec, P('row', 'col'), P('row', 'col', None, None), P()),
                         out_specs=grid_spec, check_vma=False)
```

```python
import functools
import math
import jax
import jax.numpy as jnp
from jax import lax
from jax.experimental import pallas as pl
from jax.experimental.pallas import tpu as pltpu
from jax.sharding import PartitionSpec as P

SWEEPS = 6
MESH = pl.DeviceIdType.MESH
DIRS = ((-1, 0), (1, 0), (0, -1), (0, 1), (-1, -1), (-1, 1), (1, -1), (1, 1))
BACK = (1, 0, 3, 2, 7, 6, 5, 4)
N, S, W, E, NW, NE, SW, SE = range(8)
F32, BF16 = jnp.float32, jnp.bfloat16


def kernel(geo, w_hbm, f_hbm, u_hbm, k_hbm, a_hbm, u,
           mat, r, ext, zf, cs, cw, ce, kp, kraw, knb,
           ucol, urow_in, ucol_in, w_smem,
           zo, st, st_c, h_v, h_h, h_c,
           load_sem, u_send, u_recv, k_send, k_recv, r_send, r_recv, z_send, z_recv):
    row_count, col_count, sub, halo, rhs = geo
    big = sub + 2 * halo
    tiles = sub // 8
    row, col = lax.axis_index('row'), lax.axis_index('col')

    def exists(d):
        dr, dc = DIRS[d]
        conds = []
        if dr == -1:
            conds.append(row > 0)
        if dr == 1:
            conds.append(row < row_count - 1)
        if dc == -1:
            conds.append(col > 0)
        if dc == 1:
            conds.append(col < col_count - 1)
        return functools.reduce(jnp.logical_and, conds)

    def device(d):
        dr, dc = DIRS[d]
        return {'row': row + dr, 'col': col + dc}

    def each(fn, dirs=range(8)):
        for d in dirs:
            pl.when(exists(d))(functools.partial(fn, d))

    cells, edge = sub * sub, (halo + 1) * sub
    loads = [pltpu.make_async_copy(k_hbm, kraw, load_sem.at[0]),
             pltpu.make_async_copy(u_hbm, u, load_sem.at[1]),
             pltpu.make_async_copy(f_hbm, r.at[pl.ds(halo, sub), pl.ds(halo, sub)], load_sem.at[2]),
             pltpu.make_async_copy(a_hbm.at[pl.ds(0, edge)], mat.at[pl.ds(0, edge)], load_sem.at[3]),
             pltpu.make_async_copy(a_hbm.at[pl.ds(cells - edge, edge)], mat.at[pl.ds(edge, edge)], load_sem.at[4]),
             pltpu.make_async_copy(a_hbm.at[pl.ds(edge, cells - 2 * edge)], mat.at[pl.ds(2 * edge, cells - 2 * edge)],
                                   load_sem.at[5]),
             pltpu.make_async_copy(w_hbm, w_smem, load_sem.at[6])]
    for copy in loads:
        copy.start()

    for start in (0, halo + sub):
        r[pl.ds(start, halo)] = jnp.zeros((halo, big, rhs), F32)
        r[pl.ds(halo, sub), pl.ds(start, halo)] = jnp.zeros((sub, halo, rhs), F32)
    knb[...] = jnp.zeros_like(knb)
    h_v[:, 1] = jnp.zeros((2,) + h_v.shape[2:], BF16)
    h_h[:, 1] = jnp.zeros((2,) + h_h.shape[2:], BF16)
    h_c[1] = jnp.zeros(h_c.shape[1:], BF16)

    barrier = pltpu.get_barrier_semaphore()

    def greet(d):
        pl.semaphore_signal(barrier, inc=1, device_id=device(d), device_id_type=MESH)

    each(greet)

    def zero_row(i, carry):
        zf[i] = jnp.zeros((big + 16, rhs), F32)
        return carry

    lax.fori_loop(0, big + 2, zero_row, 0)
    kp[...] = jnp.zeros_like(kp)
    loads[0].wait()
    kp[:, 0:sub] = kraw[...]
    loads[1].wait()

    def u_to_zf(i, carry):
        zf[halo + 1 + i, pl.ds(halo + 8, sub)] = u[pl.ds(pl.multiple_of(i * sub, sub), sub)]
        return carry

    lax.fori_loop(0, sub, u_to_zf, 0)
    ucol[0] = zf[pl.ds(halo + 1, sub), halo + 8, :]
    ucol[1] = zf[pl.ds(halo + 1, sub), halo + 8 + sub - 1, :]

    def band(at, count):
        return 3 - (at == 0).astype(jnp.int32) - (at == count - 1).astype(jnp.int32)

    pl.semaphore_wait(barrier, band(row, row_count) * band(col, col_count) - 1)

    def u_copy(d):
        src = {N: u.at[pl.ds(0, sub)], S: u.at[pl.ds((sub - 1) * sub, sub)],
               W: ucol.at[0], E: ucol.at[1]}[d]
        dst = {N: urow_in.at[1], S: urow_in.at[0], W: ucol_in.at[1], E: ucol_in.at[0]}[d]
        return pltpu.make_async_remote_copy(src, dst, u_send.at[d], u_recv.at[BACK[d]],
                                            device_id=device(d), device_id_type=MESH)

    def u_arrival(d):
        dst = {N: urow_in.at[0], S: urow_in.at[1], W: ucol_in.at[0], E: ucol_in.at[1]}[d]
        return pltpu.make_async_remote_copy(dst, dst, u_send.at[d], u_recv.at[d],
                                            device_id=device(d), device_id_type=MESH)

    def k_copy(d):
        return pltpu.make_async_remote_copy(kp, knb.at[BACK[d]], k_send.at[d], k_recv.at[BACK[d]],
                                            device_id=device(d), device_id_type=MESH)

    def k_arrival(d):
        return pltpu.make_async_remote_copy(knb.at[d], knb.at[d], k_send.at[d], k_recv.at[d],
                                            device_id=device(d), device_id_type=MESH)

    each(lambda d: u_copy(d).start(), (E, W, S, N))
    each(lambda d: k_copy(d).start(), (E, W, S, N, NE, NW, SE, SW))
    def block_row(left, mid, right):
        return left + pltpu.roll(mid, sub, 1) + pltpu.roll(right, 2 * sub, 1)

    j0 = sub - halo

    def faces(north, mid, south):
        kk = jnp.concatenate([north, mid, south, jnp.zeros((128 - 3 * sub, 128), F32)], axis=0)
        kt = jnp.transpose(kk)
        g_row = row * sub - sub + lax.broadcasted_iota(jnp.int32, (128, 128), 1)
        g_col = col * sub - sub + lax.broadcasted_iota(jnp.int32, (128, 128), 0)
        row_in = jnp.logical_and(g_row >= 0, g_row < row_count * sub)
        col_in = jnp.logical_and(g_col >= 0, g_col < col_count * sub)
        row_next = jnp.logical_and(g_row >= -1, g_row < row_count * sub - 1)
        col_next = jnp.logical_and(g_col >= -1, g_col < col_count * sub - 1)
        here = jnp.logical_and(row_in, col_in)
        kt = jnp.where(here, kt, 0.0)
        k_down = pltpu.roll(kt, 127, 1)
        k_right = pltpu.roll(kt, 127, 0)
        face_s = jnp.where(jnp.logical_and(here, jnp.logical_and(row_next, col_in)), 0.5, 1.0) * (kt + k_down)
        face_e = jnp.where(jnp.logical_and(here, jnp.logical_and(row_in, col_next)), 0.5, 1.0) * (kt + k_right)
        return face_s, face_e, pltpu.roll(face_e, 1, 0)

    def spread(face, i, j, width):
        lane = i + j0
        return jnp.broadcast_to(face[j0 + j:j0 + j + width, lane:lane + 1], (width, rhs))

    each(lambda d: k_arrival(d).wait_recv(), (N, S, W, E))
    zero = jnp.zeros((sub, 128), F32)
    mid = block_row(knb[W], kp[...], knb[E])
    face_s, face_e, face_w = faces(block_row(zero, knb[N], zero), mid, block_row(zero, knb[S], zero))
    own = pl.ds(halo, sub)
    for i in range(halo - 1, halo + sub):
        cs[i + 1, own] = spread(face_s, i, halo, sub)
        if i >= halo:
            cw[i, own] = spread(face_w, i, halo, sub)
            ce[i, own] = spread(face_e, i, halo, sub)

    def operator(i, j, width):
        c = zf[i + 1, pl.ds(8 + j, width)]
        span = pl.ds(j, width)
        return (cs[i, span] * (c - zf[i, pl.ds(8 + j, width)])
                + cs[i + 1, span] * (c - zf[i + 2, pl.ds(8 + j, width)])
                + cw[i, span] * (c - zf[i + 1, pl.ds(7 + j, width)])
                + ce[i, span] * (c - zf[i + 1, pl.ds(9 + j, width)]))

    def put_u(d):
        u_arrival(d).wait_recv()
        if d == N:
            zf[halo, pl.ds(halo + 8, sub)] = urow_in[0]
        if d == S:
            zf[halo + sub + 1, pl.ds(halo + 8, sub)] = urow_in[1]
        if d == W:
            zf[pl.ds(halo + 1, sub), halo + 7, :] = ucol_in[0]
        if d == E:
            zf[pl.ds(halo + 1, sub), halo + 8 + sub, :] = ucol_in[1]

    each(put_u, (N, S, W, E))
    loads[2].wait()

    def first_residual(i, carry):
        r[i, pl.ds(halo, sub)] = r[i, pl.ds(halo, sub)] - operator(i, halo, sub)
        return carry

    lax.fori_loop(halo, halo + sub, first_residual, 0, unroll=4)

    def span_of(delta, outer):
        if delta == 0:
            return pl.ds(halo, sub)
        if outer:
            return pl.ds(0, halo) if delta < 0 else pl.ds(halo + sub, halo)
        return pl.ds(halo, halo) if delta < 0 else pl.ds(sub, halo)

    def r_copy(d):
        dr, dc = DIRS[d]
        return pltpu.make_async_remote_copy(
            r.at[span_of(dr, False), span_of(dc, False)], r.at[span_of(-dr, True), span_of(-dc, True)],
            r_send.at[d], r_recv.at[BACK[d]], device_id=device(d), device_id_type=MESH)

    def r_arrival(d):
        dr, dc = DIRS[d]
        dst = r.at[span_of(dr, True), span_of(dc, True)]
        return pltpu.make_async_remote_copy(dst, dst, r_send.at[d], r_recv.at[d],
                                            device_id=device(d), device_id_type=MESH)

    depth = halo + 1
    near, far = pl.ds(0, depth), pl.ds(sub - depth, depth)
    part = {1: pl.ds(0, depth), 2: pl.ds(sub + tiles - depth, depth), 3: pl.ds(depth, sub + tiles - 2 * depth)}
    col_at = sub - depth

    def strip_row(i):
        return i if i < sub - depth else i + tiles

    def z_source(d, k, slot):
        if d in (N, S):
            return zo.at[d, slot]
        return st.at[d - W, slot, part[k]] if d in (W, E) else st_c.at[slot, d - NW]

    def z_place(d, k, slot):
        if d in (N, S):
            return h_v.at[d, slot]
        return h_h.at[d - W, slot, part[k]] if d in (W, E) else h_c.at[slot, d - NW]

    def z_copy(d, k, slot):
        return pltpu.make_async_remote_copy(
            z_source(d, k, slot), z_place(BACK[d], k, slot), z_send.at[slot, k, d], z_recv.at[slot, k, BACK[d]],
            device_id=device(d), device_id_type=MESH)

    def z_arrival(d, k, slot):
        return pltpu.make_async_remote_copy(
            z_place(d, k, slot), z_place(d, k, slot), z_send.at[slot, k, d], z_recv.at[slot, k, d],
            device_id=device(d), device_id_type=MESH)

    def ks(d):
        return (1, 2, 3) if d in (W, E) else (0,)

    left_col, right_col = halo, sub - depth
    chunks = ((0, depth), (sub - depth, depth), (depth, sub - 2 * depth))

    def stage(slot, lo, count, value, column):
        tile = value.reshape(count, tiles, 8, rhs).astype(BF16)
        at = pl.ds(strip_row(lo), count)
        st[0, slot, at] = tile[:, 0]
        st[1, slot, at] = tile[:, tiles - 1]
        if lo == 0:
            zo[N, slot] = tile
            groups, corners = (0,), (NW, NE)
        elif lo == sub - depth:
            zo[S, slot] = tile
            groups, corners = (tiles - 1,), (SW, SE)
        else:
            groups, corners = range(1, tiles - 1), ()
        for k in groups:
            st[0, slot, col_at + k] = column(8 * k, left_col).astype(BF16)
            st[1, slot, col_at + k] = column(8 * k, right_col).astype(BF16)
        for d in corners:
            side = d & 1
            st_c[slot, d - NW, pl.ds(0, depth)] = tile[:, side * (tiles - 1)]
            st_c[slot, d - NW, depth] = st[side, slot, col_at + groups[0]]

    def send(slot, los):
        dirs = []
        if 0 in los:
            dirs += [(NE, 0), (NW, 0)]
        if sub - depth in los:
            dirs += [(SE, 0), (SW, 0)]
        if 0 in los:
            dirs += [(N, 0), (E, 1), (W, 1)]
        if sub - depth in los:
            dirs += [(S, 0), (E, 2), (W, 2)]
        if depth in los:
            dirs += [(E, 3), (W, 3)]
        for d, k in dirs:
            pl.when(exists(d))(lambda: z_copy(d, k, slot).start())

    def sent(slot):
        each(lambda d: [z_copy(d, k, slot).wait_send() for k in ks(d)] and None)

    for lo, count in chunks:
        stage(1, lo, count, r[pl.ds(halo + lo, count), own],
              lambda i, j: r[pl.ds(halo + i, 8), halo + j, :])
    send(1, [lo for lo, _ in chunks])
    each(lambda d: r_copy(d).start(), (NE, NW, SE, SW, E, W, S, N))
    each(lambda d: u_copy(d).wait_send(), (N, S, W, E))
    each(lambda d: k_copy(d).wait_send())
    each(lambda d: k_arrival(d).wait_recv(), (NW, NE, SW, SE))
    face_s, face_e, face_w = faces(block_row(knb[NW], knb[N], knb[NE]), mid, block_row(knb[SW], knb[S], knb[SE]))
    for i in range(-1, big):
        inside = halo <= i < halo + sub
        for j, width in ((0, halo), (halo + sub, halo)) if inside else ((0, big),):
            span = pl.ds(j, width)
            if i == halo - 1:
                cs[i + 1, pl.ds(0, halo)] = spread(face_s, i, 0, halo)
                cs[i + 1, pl.ds(halo + sub, halo)] = spread(face_s, i, halo + sub, halo)
            else:
                cs[i + 1, span] = spread(face_s, i, j, width)
            if i >= 0:
                cw[i, span] = spread(face_w, i, j, width)
                ce[i, span] = spread(face_e, i, j, width)
    for copy in loads[3:]:
        copy.wait()
    omega = w_smem[0, 0]
    each(lambda d: [z_arrival(d, k, 1).wait_recv() for k in ks(d)] and None)
    for i in range(big):
        if i < halo:
            left, mid_r, right = h_c[1, 0, i + 1], h_v[N, 1, i + 1], h_c[1, 1, i + 1]
            mid_r = mid_r.astype(F32).reshape(sub, rhs)
        elif i < halo + sub:
            k = strip_row(i - halo)
            left, mid_r, right = h_h[0, 1, k], r[i, own], h_h[1, 1, k]
        else:
            k = i - halo - sub
            left, mid_r, right = h_c[1, 2, k], h_v[S, 1, k], h_c[1, 3, k]
            mid_r = mid_r.astype(F32).reshape(sub, rhs)
        ext[i] = jnp.concatenate([left.astype(F32), mid_r, right.astype(F32)], axis=0).astype(BF16)
    sent(1)

    k_half = 5 * 256

    def solve(group, e):
        if group == 0:
            parts = [jnp.dot(mat[pl.ds(at, edge), :], e, preferred_element_type=F32) for at in (0, edge)]
        else:
            rows = pl.ds(2 * edge, cells - 2 * edge)
            parts = [jnp.dot(mat[rows, :k_half], e[:k_half], preferred_element_type=F32)
                     + jnp.dot(mat[rows, k_half:], e[k_half:], preferred_element_type=F32)]
        parts = [z.astype(BF16).astype(F32) for z in parts]
        if group == 0:
            return (0, depth, parts[0]), (sub - depth, depth, parts[1])
        return ((depth, sub - 2 * depth, parts[0]),)

    def update(i, j, width):
        span = pl.ds(j, width)
        new = r[i, span] - omega * operator(i, j, width)
        r[i, span] = new
        ext[i, span] = new.astype(BF16)

    def sweep(t, carry):
        slot = lax.rem(t, 2)
        e = ext[...].reshape(big * big, rhs)
        for group in range(2):
            done = solve(group, e)
            for lo, count, z in done:
                z = z.reshape(count, sub, rhs)
                zf[pl.ds(halo + 1 + lo, count), pl.ds(halo + 8, sub)] = z
                stage(slot, lo, count, z, lambda i, j: zf[pl.ds(halo + 1 + i, 8), halo + 8 + j, :])
            send(slot, [lo for lo, _, _ in done])

        for i in range(sub):
            cells = pl.ds(i * sub, sub)
            u[cells] = u[cells] + omega * zf[halo + 1 + i, pl.ds(halo + 8, sub)]

        def r_ready(d):
            r_copy(d).wait_send()
            r_arrival(d).wait_recv()

        @pl.when(t == 0)
        def _():
            each(r_ready)

        for i in range(halo + 1, halo + sub - 1):
            update(i, 16, 16)

        right, below = halo + sub + 8, halo + sub + 1

        def put_z(d):
            for k in ks(d):
                z_arrival(d, k, slot).wait_recv()
            if d in (N, S):
                at = 0 if d == N else below
                zf[pl.ds(at, depth), pl.ds(halo + 8, sub)] = h_v[d, slot].astype(F32).reshape(depth, sub, rhs)
            elif d in (W, E):
                at, edge = (8, 7) if d == W else (right, right + 8)
                for lo, count in chunks:
                    zf[pl.ds(halo + 1 + lo, count), pl.ds(at, 8)] = h_h[d - W, slot, pl.ds(strip_row(lo), count)].astype(F32)
                for k in range(tiles):
                    zf[pl.ds(halo + 1 + 8 * k, 8), edge, :] = h_h[d - W, slot, col_at + k].astype(F32)
            else:
                dr, dc = DIRS[d]
                at, edge = (8, 7) if dc < 0 else (right, right + 8)
                start, edge_start = (0, 1) if dr < 0 else (below, below)
                zf[pl.ds(start, depth), pl.ds(at, 8)] = h_c[slot, d - NW, pl.ds(0, depth)].astype(F32)
                zf[pl.ds(edge_start, 8), edge, :] = h_c[slot, d - NW, depth].astype(F32)

        each(put_z, (N, S))
        for i in (*range(halo + 1), *range(halo + sub - 1, big)):
            update(i, 16, 16)

        def side(d):
            each(put_z, (NW, SW, W) if d == W else (NE, SE, E))
            for i in range(big):
                update(i, 0 if d == W else 32, 16)

        west_last = lax.rem(col, 4) == 0

        @pl.when(west_last)
        def _():
            side(E)
            side(W)

        @pl.when(jnp.logical_not(west_last))
        def _():
            side(W)
            side(E)

        sent(slot)
        return carry

    lax.fori_loop(0, SWEEPS - 1, sweep, 0)
    e = ext[...].reshape(big * big, rhs)
    for group in range(2):
        for lo, count, z in solve(group, e):
            span = pl.ds(lo * sub, count * sub)
            u[span] = u[span] + omega * z


def write_out(u_ref, out_hbm, sem):
    copy = pltpu.make_async_copy(u_ref, out_hbm, sem)
    copy.start()
    copy.wait()


def solution(mesh):
    row_count = mesh.shape['row']
    col_count = mesh.shape['col']
    grid_spec = P('row', 'col', None)

    def device_fn(f_blk, u_blk, kappa_blk, mat_blk, omega_relax):
        sub, _, rhs = u_blk.shape
        rows, cols = mat_blk.shape[2:]
        big = math.isqrt(cols)
        halo = (big - sub) // 2
        tiles = sub // 8
        dma, vmem = pltpu.SemaphoreType.DMA, pltpu.VMEM
        flat = jax.ShapeDtypeStruct((sub * sub, rhs), F32)
        u_new = pl.pallas_call(
            functools.partial(kernel, (row_count, col_count, sub, halo, rhs)),
            out_shape=pltpu.VMEM(flat.shape, F32),
            in_specs=[pl.BlockSpec(memory_space=pl.ANY)] * 5,
            out_specs=pl.BlockSpec(memory_space=pltpu.VMEM),
            scratch_shapes=[
                vmem((rows, cols), BF16), vmem((big, big, rhs), F32),
                vmem((big, big, rhs), BF16), vmem((big + 2, big + 16, rhs), F32),
                vmem((big + 1, big, rhs), F32), vmem((big, big, rhs), F32), vmem((big, big, rhs), F32),
                vmem((sub, 128), F32), vmem((sub, sub), F32), vmem((8, sub, 128), F32),
                vmem((2, sub, rhs), F32), vmem((2, sub, rhs), F32), vmem((2, sub, rhs), F32),
                pltpu.SMEM((1, 1), F32),
                vmem((2, 2, halo + 1, tiles, 8, rhs), BF16), vmem((2, 2, sub + tiles, 8, rhs), BF16),
                vmem((2, 4, halo + 2, 8, rhs), BF16),
                vmem((2, 2, halo + 1, tiles, 8, rhs), BF16), vmem((2, 2, sub + tiles, 8, rhs), BF16),
                vmem((2, 4, halo + 2, 8, rhs), BF16),
                dma((7,)), dma((4,)), dma((4,)), dma((8,)), dma((8,)), dma((8,)), dma((8,)),
                dma((2, 4, 8)), dma((2, 4, 8)),
            ],
            compiler_params=pltpu.CompilerParams(collective_id=0, has_side_effects=True),
        )(omega_relax.reshape(1, 1), f_blk, u_blk.reshape(sub * sub, rhs), kappa_blk, mat_blk.reshape(rows, cols))
        out = pl.pallas_call(
            write_out, out_shape=flat,
            in_specs=[pl.BlockSpec(memory_space=pltpu.VMEM)], out_specs=pl.BlockSpec(memory_space=pl.ANY),
            scratch_shapes=[dma],
        )(u_new)
        return out.reshape(sub, sub, rhs)

    return jax.shard_map(device_fn, mesh=mesh,
                         in_specs=(grid_spec, grid_spec, P('row', 'col'), P('row', 'col', None, None), P()),
                         out_specs=grid_spec, check_vma=False)
```

```python
import functools
import math
import jax
import jax.numpy as jnp
from jax import lax
from jax.experimental import pallas as pl
from jax.experimental.pallas import tpu as pltpu
from jax.sharding import PartitionSpec as P

SWEEPS = 6
MESH = pl.DeviceIdType.MESH
DIRS = ((-1, 0), (1, 0), (0, -1), (0, 1), (-1, -1), (-1, 1), (1, -1), (1, 1))
BACK = (1, 0, 3, 2, 7, 6, 5, 4)
N, S, W, E, NW, NE, SW, SE = range(8)
F32, BF16 = jnp.float32, jnp.bfloat16


def kernel(geo, w_hbm, f_hbm, u_hbm, k_hbm, a_hbm, u, z_last,
           mat, r, ext, zf, cs, cw, ce, kp, kraw, knb,
           ucol, urow_in, ucol_in, w_smem,
           zo, st_a, st_b, st_c, h_v, h_a, h_b, h_c,
           load_sem, u_send, u_recv, k_send, k_recv, r_send, r_recv, z_send, z_recv):
    row_count, col_count, sub, halo, rhs = geo
    big = sub + 2 * halo
    tiles = sub // 8
    row, col = lax.axis_index('row'), lax.axis_index('col')

    def exists(d):
        dr, dc = DIRS[d]
        conds = []
        if dr == -1:
            conds.append(row > 0)
        if dr == 1:
            conds.append(row < row_count - 1)
        if dc == -1:
            conds.append(col > 0)
        if dc == 1:
            conds.append(col < col_count - 1)
        return functools.reduce(jnp.logical_and, conds)

    def device(d):
        dr, dc = DIRS[d]
        return {'row': row + dr, 'col': col + dc}

    def each(fn, dirs=range(8)):
        for d in dirs:
            pl.when(exists(d))(functools.partial(fn, d))

    cells, edge = sub * sub, (halo + 1) * sub
    loads = [pltpu.make_async_copy(k_hbm, kraw, load_sem.at[0]),
             pltpu.make_async_copy(u_hbm, u, load_sem.at[1]),
             pltpu.make_async_copy(f_hbm, r.at[pl.ds(halo, sub), pl.ds(halo, sub)], load_sem.at[2]),
             pltpu.make_async_copy(a_hbm.at[pl.ds(0, edge)], mat.at[pl.ds(0, edge)], load_sem.at[3]),
             pltpu.make_async_copy(a_hbm.at[pl.ds(cells - edge, edge)], mat.at[pl.ds(edge, edge)], load_sem.at[4]),
             pltpu.make_async_copy(a_hbm.at[pl.ds(edge, cells - 2 * edge)], mat.at[pl.ds(2 * edge, cells - 2 * edge)],
                                   load_sem.at[5]),
             pltpu.make_async_copy(w_hbm, w_smem, load_sem.at[6])]
    for copy in loads:
        copy.start()

    for start in (0, halo + sub):
        r[pl.ds(start, halo)] = jnp.zeros((halo, big, rhs), F32)
        r[pl.ds(halo, sub), pl.ds(start, halo)] = jnp.zeros((sub, halo, rhs), F32)
    knb[...] = jnp.zeros_like(knb)
    h_v[:, 1] = jnp.zeros((2,) + h_v.shape[2:], BF16)
    h_a[:, 1] = jnp.zeros((2,) + h_a.shape[2:], BF16)
    h_b[:, 1] = jnp.zeros((2,) + h_b.shape[2:], BF16)
    st_c[...] = jnp.zeros_like(st_c)
    h_c[1] = jnp.zeros(h_c.shape[1:], BF16)

    barrier = pltpu.get_barrier_semaphore()

    def greet(d):
        pl.semaphore_signal(barrier, inc=1, device_id=device(d), device_id_type=MESH)

    each(greet)

    def zero_row(i, carry):
        zf[i] = jnp.zeros((big + 16, rhs), F32)
        return carry

    lax.fori_loop(0, big + 2, zero_row, 0)
    kp[...] = jnp.zeros_like(kp)
    loads[0].wait()
    kp[:, 0:sub] = kraw[...]
    loads[1].wait()

    ucol[0] = u[pl.ds(0, sub, stride=sub)]
    ucol[1] = u[pl.ds(sub - 1, sub, stride=sub)]

    def band(at, count):
        return 3 - (at == 0).astype(jnp.int32) - (at == count - 1).astype(jnp.int32)

    pl.semaphore_wait(barrier, band(row, row_count) * band(col, col_count) - 1)

    def u_copy(d):
        src = {N: u.at[pl.ds(0, sub)], S: u.at[pl.ds((sub - 1) * sub, sub)],
               W: ucol.at[0], E: ucol.at[1]}[d]
        dst = {N: urow_in.at[1], S: urow_in.at[0], W: ucol_in.at[1], E: ucol_in.at[0]}[d]
        return pltpu.make_async_remote_copy(src, dst, u_send.at[d], u_recv.at[BACK[d]],
                                            device_id=device(d), device_id_type=MESH)

    def u_arrival(d):
        dst = {N: urow_in.at[0], S: urow_in.at[1], W: ucol_in.at[0], E: ucol_in.at[1]}[d]
        return pltpu.make_async_remote_copy(dst, dst, u_send.at[d], u_recv.at[d],
                                            device_id=device(d), device_id_type=MESH)

    def k_copy(d):
        return pltpu.make_async_remote_copy(kp, knb.at[BACK[d]], k_send.at[d], k_recv.at[BACK[d]],
                                            device_id=device(d), device_id_type=MESH)

    def k_arrival(d):
        return pltpu.make_async_remote_copy(knb.at[d], knb.at[d], k_send.at[d], k_recv.at[d],
                                            device_id=device(d), device_id_type=MESH)

    each(lambda d: u_copy(d).start(), (E, W, S, N))
    each(lambda d: k_copy(d).start(), (E, W, S, N, NE, NW, SE, SW))

    def u_to_zf(i, carry):
        zf[halo + 1 + i, pl.ds(halo + 8, sub)] = u[pl.ds(pl.multiple_of(i * sub, sub), sub)]
        return carry

    lax.fori_loop(0, sub, u_to_zf, 0, unroll=8)
    def block_row(left, mid, right):
        return left + pltpu.roll(mid, sub, 1) + pltpu.roll(right, 2 * sub, 1)

    j0 = sub - halo

    def faces(north, mid, south):
        kk = jnp.concatenate([north, mid, south, jnp.zeros((128 - 3 * sub, 128), F32)], axis=0)
        kt = jnp.transpose(kk)
        g_row = row * sub - sub + lax.broadcasted_iota(jnp.int32, (128, 128), 1)
        g_col = col * sub - sub + lax.broadcasted_iota(jnp.int32, (128, 128), 0)
        row_in = jnp.logical_and(g_row >= 0, g_row < row_count * sub)
        col_in = jnp.logical_and(g_col >= 0, g_col < col_count * sub)
        row_next = jnp.logical_and(g_row >= -1, g_row < row_count * sub - 1)
        col_next = jnp.logical_and(g_col >= -1, g_col < col_count * sub - 1)
        here = jnp.logical_and(row_in, col_in)
        kt = jnp.where(here, kt, 0.0)
        k_down = pltpu.roll(kt, 127, 1)
        k_right = pltpu.roll(kt, 127, 0)
        face_s = jnp.where(jnp.logical_and(here, jnp.logical_and(row_next, col_in)), 0.5, 1.0) * (kt + k_down)
        face_e = jnp.where(jnp.logical_and(here, jnp.logical_and(row_in, col_next)), 0.5, 1.0) * (kt + k_right)
        return face_s, face_e, pltpu.roll(face_e, 1, 0)

    def spread(face, i, j, width):
        lane = i + j0
        return jnp.broadcast_to(face[j0 + j:j0 + j + width, lane:lane + 1], (width, rhs))

    zero = jnp.zeros((sub, 128), F32)
    own = pl.ds(halo, sub)
    face_s, face_e, face_w = faces(zero, block_row(zero, kp[...], zero), zero)
    for i in range(halo, halo + sub):
        if i < halo + sub - 1:
            cs[i + 1, own] = spread(face_s, i, halo, sub)
        cw[i, own] = spread(face_w, i, halo, sub)
        ce[i, own] = spread(face_e, i, halo, sub)

    def operator(i, j, width):
        c = zf[i + 1, pl.ds(8 + j, width)]
        span = pl.ds(j, width)
        return (cs[i, span] * (c - zf[i, pl.ds(8 + j, width)])
                + cs[i + 1, span] * (c - zf[i + 2, pl.ds(8 + j, width)])
                + cw[i, span] * (c - zf[i + 1, pl.ds(7 + j, width)])
                + ce[i, span] * (c - zf[i + 1, pl.ds(9 + j, width)]))

    def put_u(d):
        u_arrival(d).wait_recv()
        if d == N:
            zf[halo, pl.ds(halo + 8, sub)] = urow_in[0]
        if d == S:
            zf[halo + sub + 1, pl.ds(halo + 8, sub)] = urow_in[1]
        if d == W:
            zf[pl.ds(halo + 1, sub), halo + 7, :] = ucol_in[0]
        if d == E:
            zf[pl.ds(halo + 1, sub), halo + 8 + sub, :] = ucol_in[1]

    loads[2].wait()

    def first_residual(i, j, width):
        span = pl.ds(j, width)
        r[i, span] = r[i, span] - operator(i, j, width)

    for i in range(halo + 1, halo + sub - 1):
        first_residual(i, 16, 16)
    each(lambda d: k_arrival(d).wait_recv(), (N, S, W, E))
    mid = block_row(knb[W], kp[...], knb[E])
    face_s, face_e, face_w = faces(block_row(zero, knb[N], zero), mid, block_row(zero, knb[S], zero))
    for i in (halo - 1, halo + sub - 1):
        cs[i + 1, own] = spread(face_s, i, halo, sub)
    for i in range(halo, halo + sub):
        cw[i, pl.ds(halo, 8)] = spread(face_w, i, halo, 8)
        ce[i, pl.ds(halo + sub - 8, 8)] = spread(face_e, i, halo + sub - 8, 8)
    each(put_u, (N, S, W, E))
    for i in range(halo, halo + sub):
        if i in (halo, halo + sub - 1):
            first_residual(i, halo, sub)
        else:
            first_residual(i, halo, 8)
            first_residual(i, halo + sub - 8, 8)

    def span_of(delta, outer):
        if delta == 0:
            return pl.ds(halo, sub)
        if outer:
            return pl.ds(0, halo) if delta < 0 else pl.ds(halo + sub, halo)
        return pl.ds(halo, halo) if delta < 0 else pl.ds(sub, halo)

    def r_copy(d):
        dr, dc = DIRS[d]
        return pltpu.make_async_remote_copy(
            r.at[span_of(dr, False), span_of(dc, False)], r.at[span_of(-dr, True), span_of(-dc, True)],
            r_send.at[d], r_recv.at[BACK[d]], device_id=device(d), device_id_type=MESH)

    def r_arrival(d):
        dr, dc = DIRS[d]
        dst = r.at[span_of(dr, True), span_of(dc, True)]
        return pltpu.make_async_remote_copy(dst, dst, r_send.at[d], r_recv.at[d],
                                            device_id=device(d), device_id_type=MESH)

    depth = halo + 1
    left_col, right_col = halo, sub - depth
    chunks = ((0, depth), (sub - depth, depth), (depth, sub - 2 * depth))
    lanes = 128 - rhs

    def pack(tile):
        t = tile.reshape(tile.shape[0] // 4, 4, 8, rhs)
        last = jnp.stack([t[:, 3, :, k * lanes:(k + 1) * lanes] for k in range(3)], axis=1)
        return jnp.concatenate([t[:, :3], last], axis=-1).reshape(-1, 8, 128).astype(BF16)

    def unpack(packed):
        p = packed.astype(F32).reshape(-1, 3, 8, 128)
        last = jnp.concatenate([p[:, k, :, rhs:] for k in range(3)], axis=-1)
        return jnp.concatenate([p[:, :, :, :rhs], last[:, None]], axis=1).reshape(-1, 8, rhs)

    def z_source(d, k, slot):
        if d in (N, S):
            return zo.at[d, slot]
        return (st_a, st_b)[k].at[d - W, slot] if d in (W, E) else st_c.at[slot, d - NW]

    def z_place(d, k, slot):
        if d in (N, S):
            return h_v.at[d, slot]
        return (h_a, h_b)[k].at[d - W, slot] if d in (W, E) else h_c.at[slot, d - NW]

    def z_copy(d, k, slot):
        return pltpu.make_async_remote_copy(
            z_source(d, k, slot), z_place(BACK[d], k, slot), z_send.at[slot, k, d], z_recv.at[slot, k, BACK[d]],
            device_id=device(d), device_id_type=MESH)

    def z_arrival(d, k, slot):
        return pltpu.make_async_remote_copy(
            z_place(d, k, slot), z_place(d, k, slot), z_send.at[slot, k, d], z_recv.at[slot, k, d],
            device_id=device(d), device_id_type=MESH)

    def ks(d):
        return (0, 1) if d in (W, E) else (0,)

    def start(slot, messages):
        for d, k in messages:
            pl.when(exists(d))(lambda: z_copy(d, k, slot).start())

    def stage_ends(slot, near, far, column):
        for side, (d_near, d_far) in enumerate(((NW, SW), (NE, SE))):
            cells8 = slice(side * (sub - 8), side * (sub - 8) + 8)
            t_near, t_far = near[:, cells8], far[:, cells8]
            j = (left_col, right_col)[side]
            extra = (t_near[halo:], t_far[:1], column(0, j)[None], column(sub - 8, j)[None])
            packed = pack(jnp.concatenate([t_near[:halo], t_far[1:], *extra], axis=0))
            third = 3 * halo // 4
            st_a[side, slot] = packed
            for d, at, raw in ((d_near, 0, (0, 2)), (d_far, third, (1, 3))):
                st_c[slot, d - NW, pl.ds(0, third)] = packed[at:at + third]
                for n, k in enumerate(raw):
                    st_c[slot, d - NW, third + n, :, pl.ds(0, rhs)] = extra[k][0].astype(BF16)
        zo[N, slot] = near.reshape(depth, tiles, 8, rhs).astype(BF16)
        zo[S, slot] = far.reshape(depth, tiles, 8, rhs).astype(BF16)
        start(slot, ((NE, 0), (NW, 0), (SE, 0), (SW, 0), (E, 0), (W, 0), (N, 0), (S, 0)))

    def stage_middle(slot, middle, column):
        for side in range(2):
            j = (left_col, right_col)[side]
            inner = [column(8 * k, j)[None] for k in range(1, tiles - 1)]
            st_b[side, slot] = pack(jnp.concatenate([middle[:, side * (sub - 8):side * (sub - 8) + 8], *inner], axis=0))
        start(slot, ((E, 1), (W, 1)))

    def strip_parts(side, slot):
        a, b = unpack(h_a[side, slot]), unpack(h_b[side, slot])
        inner = sub - 2 * depth
        rows = [(0, a[:halo]), (halo, a[2 * halo:2 * halo + 1]), (depth, b[:inner]),
                (sub - depth, a[2 * halo + 1:2 * halo + 2]), (sub - halo, a[halo:2 * halo])]
        cols = [(0, a[2 * halo + 2]), (sub - 8, a[2 * halo + 3])]
        cols += [(8 * k, b[inner + k - 1]) for k in range(1, tiles - 1)]
        return rows, cols

    def corner_parts(d, slot):
        third = 3 * halo // 4
        rows = unpack(h_c[slot, d - NW, pl.ds(0, third)])
        row, column = [h_c[slot, d - NW, third + n, :, pl.ds(0, rhs)].astype(F32) for n in range(2)]
        return jnp.concatenate([row[None], rows] if d in (NW, NE) else [rows, row[None]], axis=0), column

    def sent(slot):
        each(lambda d: [z_copy(d, k, slot).wait_send() for k in ks(d)] and None)

    near_r, far_r, middle_r = [r[pl.ds(halo + lo, count), own] for lo, count in chunks]

    def r_column(i, j):
        return r[pl.ds(halo + i, 8), halo + j, :]

    stage_ends(1, near_r, far_r, r_column)
    stage_middle(1, middle_r, r_column)
    each(lambda d: r_copy(d).start(), (NE, NW, SE, SW, E, W, S, N))
    each(lambda d: u_copy(d).wait_send(), (N, S, W, E))
    each(lambda d: k_copy(d).wait_send())
    each(lambda d: k_arrival(d).wait_recv(), (NW, NE, SW, SE))
    face_s, face_e, face_w = faces(block_row(knb[NW], knb[N], knb[NE]), mid, block_row(knb[SW], knb[S], knb[SE]))
    for i in range(-1, big):
        inside = halo <= i < halo + sub
        for j, width in ((0, halo), (halo + sub, halo)) if inside else ((0, big),):
            span = pl.ds(j, width)
            if i == halo - 1:
                cs[i + 1, pl.ds(0, halo)] = spread(face_s, i, 0, halo)
                cs[i + 1, pl.ds(halo + sub, halo)] = spread(face_s, i, halo + sub, halo)
            else:
                cs[i + 1, span] = spread(face_s, i, j, width)
            if i >= 0:
                cw[i, span] = spread(face_w, i, j, width)
                ce[i, span] = spread(face_e, i, j, width)
    for copy in loads[3:]:
        copy.wait()
    omega = w_smem[0, 0]
    each(lambda d: [z_arrival(d, k, 1).wait_recv() for k in ks(d)] and None)
    strips = [strip_parts(side, 1)[0] for side in range(2)]
    strips = [jnp.concatenate([t for _, t in rows], axis=0) for rows in strips]
    corner = {d: corner_parts(d, 1)[0] for d in (NW, NE, SW, SE)}
    for i in range(big):
        if i < halo:
            left, right = corner[NW][i + 1], corner[NE][i + 1]
            middle = h_v[N, 1, i + 1].astype(F32).reshape(sub, rhs)
        elif i < halo + sub:
            left, middle, right = strips[0][i - halo], r[i, own], strips[1][i - halo]
        else:
            k = i - halo - sub
            left, right = corner[SW][k], corner[SE][k]
            middle = h_v[S, 1, k].astype(F32).reshape(sub, rhs)
        ext[i] = jnp.concatenate([left, middle, right], axis=0).astype(BF16)
    sent(1)

    def dots(at, count, e, cuts):
        return sum(jnp.dot(mat[pl.ds(at, count), lo:hi], e[lo:hi], preferred_element_type=F32)
                   for lo, hi in zip(cuts[:-1], cuts[1:]))

    middle_rows = cells - 2 * edge

    def solve_ends(e):
        return [dots(at, edge, e, (0, big * big)).astype(BF16) for at in (0, edge)]

    def update(i, j, width):
        span = pl.ds(j, width)
        new = r[i, span] - omega * operator(i, j, width)
        r[i, span] = new
        ext[i, span] = new.astype(BF16)

    def sweep(t, carry):
        slot = lax.rem(t, 2)
        e = ext[...].reshape(big * big, rhs)
        def z_column(i, j):
            return zf[pl.ds(halo + 1 + i, 8), halo + 8 + j, :]

        def keep(lo, count, z):
            z = z.astype(F32).reshape(count, sub, rhs)
            zf[pl.ds(halo + 1 + lo, count), pl.ds(halo + 8, sub)] = z
            return z

        ends = [dots(at, edge, e, (0, big * big)) for at in (0, edge)]
        ends = [keep(lo, depth, z.astype(BF16)) for lo, z in zip((0, sub - depth), ends)]
        stage_ends(slot, *ends, z_column)
        middle = dots(2 * edge, middle_rows, e, (0, big * big))
        stage_middle(slot, keep(depth, sub - 2 * depth, middle.astype(BF16)), z_column)

        for i in range(sub):
            span = pl.ds(i * sub, sub)
            u[span] = u[span] + omega * zf[halo + 1 + i, pl.ds(halo + 8, sub)]

        def r_ready(d):
            r_copy(d).wait_send()
            r_arrival(d).wait_recv()

        @pl.when(t == 0)
        def _():
            each(r_ready)

        for i in range(halo + 1, halo + sub - 1):
            update(i, 16, 16)

        right, below = halo + sub + 8, halo + sub + 1

        def put_z(d):
            for k in ks(d):
                z_arrival(d, k, slot).wait_recv()
            if d in (N, S):
                at = 0 if d == N else below
                zf[pl.ds(at, depth), pl.ds(halo + 8, sub)] = h_v[d, slot].astype(F32).reshape(depth, sub, rhs)
            elif d in (W, E):
                at, edge_at = (8, 7) if d == W else (right, right + 8)
                rows, cols = strip_parts(d - W, slot)
                for lo, t in rows:
                    zf[pl.ds(halo + 1 + lo, t.shape[0]), pl.ds(at, 8)] = t
                for lo, t in cols:
                    zf[pl.ds(halo + 1 + lo, 8), edge_at, :] = t
            else:
                dr, dc = DIRS[d]
                at, edge_at = (8, 7) if dc < 0 else (right, right + 8)
                start_at, edge_start = (0, 1) if dr < 0 else (below, below)
                rows, column = corner_parts(d, slot)
                zf[pl.ds(start_at, depth), pl.ds(at, 8)] = rows
                zf[pl.ds(edge_start, 8), edge_at, :] = column

        each(put_z, (N, S))
        for i in (*range(halo + 1), *range(halo + sub - 1, big)):
            update(i, 16, 16)

        def side(d):
            each(put_z, (NW, SW, W) if d == W else (NE, SE, E))
            for i in range(big):
                update(i, 0 if d == W else 32, 16)

        west_last = lax.rem(col, 4) == 0

        @pl.when(west_last)
        def _():
            side(E)
            side(W)

        @pl.when(jnp.logical_not(west_last))
        def _():
            side(W)
            side(E)

        sent(slot)
        return carry

    lax.fori_loop(0, SWEEPS - 1, sweep, 0)
    e = ext[...].reshape(big * big, rhs)
    near, far = solve_ends(e)
    z_last[pl.ds(0, edge)] = near
    z_last[pl.ds(cells - edge, edge)] = far
    z_last[pl.ds(edge, middle_rows)] = dots(2 * edge, middle_rows, e, (0, 1280, big * big)).astype(BF16)


def solution(mesh):
    row_count = mesh.shape['row']
    col_count = mesh.shape['col']
    grid_spec = P('row', 'col', None)

    def device_fn(f_blk, u_blk, kappa_blk, mat_blk, omega_relax):
        sub, _, rhs = u_blk.shape
        rows, cols = mat_blk.shape[2:]
        big = math.isqrt(cols)
        halo = (big - sub) // 2
        tiles = sub // 8
        dma, vmem = pltpu.SemaphoreType.DMA, pltpu.VMEM
        first, second = 2 * (halo + 1) + 2, sub - 2 * (halo + 1) + tiles - 2
        buffers = [vmem((2, 2, halo + 1, tiles, 8, rhs), BF16), vmem((2, 2, 3 * first // 4, 8, 128), BF16),
                   vmem((2, 2, 3 * second // 4, 8, 128), BF16), vmem((2, 4, 3 * halo // 4 + 2, 8, 128), BF16)]
        u_new, z_last = pl.pallas_call(
            functools.partial(kernel, (row_count, col_count, sub, halo, rhs)),
            out_shape=(pltpu.VMEM((sub * sub, rhs), F32), pltpu.VMEM((sub * sub, rhs), BF16)),
            in_specs=[pl.BlockSpec(memory_space=pl.ANY)] * 5,
            out_specs=[pl.BlockSpec(memory_space=pltpu.VMEM)] * 2,
            scratch_shapes=[
                vmem((rows, cols), BF16), vmem((big, big, rhs), F32),
                vmem((big, big, rhs), BF16), vmem((big + 2, big + 16, rhs), F32),
                vmem((big + 1, big, rhs), F32), vmem((big, big, rhs), F32), vmem((big, big, rhs), F32),
                vmem((sub, 128), F32), vmem((sub, sub), F32), vmem((8, sub, 128), F32),
                vmem((2, sub, rhs), F32), vmem((2, sub, rhs), F32), vmem((2, sub, rhs), F32),
                pltpu.SMEM((1, 1), F32),
                *buffers,
                *buffers,
                dma((7,)), dma((4,)), dma((4,)), dma((8,)), dma((8,)), dma((8,)), dma((8,)),
                dma((2, 2, 8)), dma((2, 2, 8)),
            ],
            compiler_params=pltpu.CompilerParams(collective_id=0, has_side_effects=True),
        )(omega_relax.reshape(1, 1), f_blk, u_blk.reshape(sub * sub, rhs), kappa_blk, mat_blk.reshape(rows, cols))
        out = u_new + omega_relax * z_last.astype(F32)
        return out.reshape(sub, sub, rhs)

    return jax.shard_map(device_fn, mesh=mesh,
                         in_specs=(grid_spec, grid_spec, P('row', 'col'), P('row', 'col', None, None), P()),
                         out_specs=grid_spec, check_vma=False)
```
